32 devices in a mesh: sfc: 16 (over z, y, x), grp: 2 (over core).
Axes of the slice: x: 2, y: 2, z: 4, core: 2. Of those that a mesh axis runs over, the one named last changes fastest.
Arguments:
- right_side: float32 [5, 5, 5, 4096], P(None, None, None, ('sfc', 'grp')), may hold values from -8 to 8
- cell_level: int32 [4096], P(('sfc', 'grp')), may hold values from 0 to 3
- own_slot: int32 [12288], P(('sfc', 'grp')), may hold values from 0 to 767
- near_slot: int32 [12288], P(('sfc', 'grp')), may hold values from 0 to 1151, as said below
- face_kind: int32 [12288], P(('sfc', 'grp')), may hold values from 0 to 5
- orientation: int32 [12288], P(('sfc', 'grp')), may hold values from 0 to 7
- penalty: float32 [12288], P(('sfc', 'grp')), may hold values from 2 to 32
- send_slots: int32 [12288], P(('sfc', 'grp')), may hold values from 0 to 767
- subface_maps: float32 [4, 25, 25], replicated, may hold values from -1.25 to 1.25
Outputs:
- solution: float32 [5, 5, 5, 4096], P(None, None, None, ('sfc', 'grp'))
- residual: float32 [5, 5, 5, 4096], P(None, None, None, ('sfc', 'grp'))
The draws below stay inside these ranges and needn't reach their ends.
Inputs may be any that keep to these rules, and one draw needn't show every extreme that they name: `own_slot`: a face slot f * 128 + c of the same device. `near_slot`: 768 + k * 96 + i for position i of the received block k; since a device has exactly 384 entries, its near slots are a permutation of its 384 received positions. `face_kind`: 0 boundary face, 1 conforming face, 2 + s the fine side of a hanging face with subface s. `send_slots`: a device's entries k * 96 to k * 96 + 95 are face slots of its own cells sent to the device at offset (+1, -1, +2, -2)[k].
All inputs are finite; a program needn't handle non-finite values.
Results may differ from the reference program's by a relative error of at most 0.00021.
Values sent between devices are 32-bit elements; how exact they have to be, the bound alone decides.
A program may use at most 64 MiB of HBM per device.

```python
import math
import jax
import jax.numpy as jnp
import numpy as np
from jax import lax

NODES = 5
CELLS_DEV = 128
GHOST = 96
ITERS = 3
ENTRY_DEV = 384
CELLS = 4096
ENTRIES = 12288
SENDS = 12288
N_SFC = 16
N_GRP = 2


def draw_right_side(key, part):
    position = jnp.arange(CELLS, dtype=jnp.float32) / CELLS
    values = jax.random.normal(key, (NODES, NODES, NODES, CELLS), jnp.float32)
    return jnp.clip(values, -4.0, 4.0) * jnp.sqrt(1.0 + 2.0 * position)


def draw_near_slot(key, part):
    devices = ENTRIES // ENTRY_DEV
    received = 4 * GHOST
    local_key = jax.random.fold_in(key, 11)
    order_key = jax.random.fold_in(key, 23)
    local = jax.random.randint(local_key, (devices, ENTRY_DEV), 0, 6 * CELLS_DEV, dtype=jnp.int32)
    device_keys = jax.random.split(order_key, devices)
    order = jax.vmap(lambda single: jax.random.permutation(single, ENTRY_DEV))(device_keys).astype(jnp.int32)
    chosen = jnp.where(order < received, 6 * CELLS_DEV + order, local)
    return chosen.reshape(-1).astype(jnp.int32)


def place_ends(drawn, stream_key, smallest, largest):
    longest = drawn.shape.index(max(drawn.shape))
    spots = []
    for shift in (0, 1):
        where = [jax.random.randint(jax.random.fold_in(stream_key, axis), (), 0, length) for axis, length in enumerate(drawn.shape)]
        where[longest] = (where[longest] + shift) % drawn.shape[longest]
        spots.append(tuple(where))
    return drawn.at[spots[0]].set(smallest).at[spots[1]].set(largest)


def block_levels(own_key, shape, cuts, least, largest):
    loudness, own = 1.0, jax.random.fold_in(own_key, 6)
    for dim, blocks in cuts:
        heights = jnp.exp(jax.random.uniform(jax.random.fold_in(own, dim), (blocks,), jnp.float32, least / len(cuts), largest / len(cuts)))
        loudness = loudness * jnp.repeat(heights, shape[dim] // blocks).reshape([-1 if axis == dim else 1 for axis in range(len(shape))])
    return loudness


def centred(rng, shape, scale, reach, kind=jnp.bfloat16):
    values = jax.random.normal(rng, shape, jnp.float32) * scale
    return jnp.minimum(jnp.maximum(values, -reach), reach).astype(kind)


def setup_inputs(seed: int = 0) -> dict:
    seeds = jax.random.split(jax.random.key(seed), 10)
    right_side = draw_right_side(jax.random.fold_in(seeds[9], 71), 0)
    cell_level = place_ends(jax.random.randint(seeds[1], (CELLS,), 0, 4), jax.random.fold_in(seeds[1], 1), 0, 3).astype(jnp.int32)
    own_slot = place_ends(jax.random.randint(seeds[2], (ENTRIES,), 0, 6 * CELLS_DEV), jax.random.fold_in(seeds[2], 1), 0, (6 * CELLS_DEV) - 1).astype(jnp.int32)
    near_slot = draw_near_slot(jax.random.fold_in(seeds[9], 71), 0)
    face_kind = place_ends(jax.random.randint(seeds[4], (ENTRIES,), 0, 6), jax.random.fold_in(seeds[4], 1), 0, 5).astype(jnp.int32)
    orientation = place_ends(jax.random.randint(seeds[5], (ENTRIES,), 0, 8), jax.random.fold_in(seeds[5], 1), 0, 7).astype(jnp.int32)
    penalty = jnp.clip(jnp.exp(math.log(32.0) - 2.7725887 * jax.random.uniform(seeds[6], (ENTRIES,), jnp.float32) ** block_levels(seeds[6], (ENTRIES,), ((0, 32),), -0.2, 0.2)), 2.0, 32.0)
    send_slots = place_ends(jax.random.randint(seeds[7], (SENDS,), 0, 6 * CELLS_DEV), jax.random.fold_in(seeds[7], 1), 0, (6 * CELLS_DEV) - 1).astype(jnp.int32)
    subface_maps = centred(seeds[8], (4, NODES * NODES, NODES * NODES), (NODES * NODES) ** -0.5, 1.25, jnp.float32)
    return dict(right_side=right_side, cell_level=cell_level, own_slot=own_slot, near_slot=near_slot, face_kind=face_kind, orientation=orientation, penalty=penalty, send_slots=send_slots, subface_maps=subface_maps)


mass_shift = 1.0
curve_offsets = (1, -1, 2, -2)

def node_tables():
    points = np.array([-1.0, -np.sqrt(3.0 / 7.0), 0.0, np.sqrt(3.0 / 7.0), 1.0])
    weights = np.array([0.1, 49.0 / 90.0, 32.0 / 45.0, 49.0 / 90.0, 0.1])
    identity = np.eye(5)
    spacing = points[:, None] - points[None, :] + identity
    barycentric = 1.0 / np.prod(spacing, axis=1)
    offdiag = barycentric[None, :] / barycentric[:, None] / spacing
    diagonal = np.sum(1.0 / spacing, axis=1) - 1.0
    derivs = np.where(identity > 0.5, diagonal[:, None], offdiag)
    stiffness = derivs.T @ (weights[:, None] * derivs)
    return (jnp.asarray(stiffness, jnp.float32), jnp.asarray(weights, jnp.float32))

def volume_term(field, scale, tables):
    stiffness, weights = tables
    first = weights[:, None, None, None]
    second = weights[None, :, None, None]
    third = weights[None, None, :, None]
    along_first = jnp.einsum('ia,abcz->ibcz', stiffness, field, precision=lax.Precision.HIGHEST)
    along_second = jnp.einsum('jb,abcz->ajcz', stiffness, field, precision=lax.Precision.HIGHEST)
    along_third = jnp.einsum('kc,abcz->abkz', stiffness, field, precision=lax.Precision.HIGHEST)
    grads = along_first * second * third + along_second * first * third + along_third * first * second
    return scale * grads + mass_shift * scale * scale * scale * first * second * third * field

def face_traces(field):
    last = NODES - 1
    return jnp.stack([field[0], field[last], field[:, 0], field[:, last], field[:, :, 0], field[:, :, last]], axis=-2)

def lift_faces(faces):
    last = NODES - 1
    rest = faces.shape[2:-2] + faces.shape[-1:]
    volume = jnp.zeros((NODES, NODES, NODES) + rest, faces.dtype)
    volume = volume.at[0].add(faces[..., 0, :])
    volume = volume.at[last].add(faces[..., 1, :])
    volume = volume.at[:, 0].add(faces[..., 2, :])
    volume = volume.at[:, last].add(faces[..., 3, :])
    volume = volume.at[:, :, 0].add(faces[..., 4, :])
    volume = volume.at[:, :, last].add(faces[..., 5, :])
    return volume

def orient_forward(values, codes):
    values = jnp.where(codes & 1 == 1, values[::-1], values)
    values = jnp.where(codes & 2 == 2, values[:, ::-1], values)
    return jnp.where(codes & 4 == 4, jnp.swapaxes(values, 0, 1), values)

def orient_back(values, codes):
    values = jnp.where(codes & 4 == 4, jnp.swapaxes(values, 0, 1), values)
    values = jnp.where(codes & 2 == 2, values[:, ::-1], values)
    return jnp.where(codes & 1 == 1, values[::-1], values)

def map_traces(values, kinds, maps, transpose_maps):
    flat = values.reshape(NODES * NODES, -1)
    result = jnp.where(kinds == 1, flat, 0.0)
    for subface in range(4):
        matrix = maps[subface].T if transpose_maps else maps[subface]
        moved = jnp.dot(matrix, flat, precision=lax.Precision.HIGHEST)
        result = result + jnp.where(kinds == subface + 2, moved, 0.0)
    return result.reshape(values.shape)

def face_terms(own_values, near_values, kinds, orients, penalty, maps, weights):
    face_mass = weights[:, None, None] * weights[None, :, None]
    mapped = map_traces(orient_forward(near_values, orients), kinds, maps, False)
    jump = own_values - mapped
    own_term = penalty * face_mass * jump
    near_term = -orient_back(map_traces(own_term, kinds, maps, True), orients)
    return (own_term, near_term)

def shift_devices(blocks, offset):
    empty = jnp.zeros_like(blocks[:, :abs(offset)])
    if offset > 0:
        return jnp.concatenate([empty, blocks[:, :-offset]], axis=1)
    return jnp.concatenate([blocks[:, -offset:], empty], axis=1)

def apply_operator(field, scale, own_slot, near_slot, kinds, orients, penalty, send_slots, maps, tables):
    devices = N_SFC * N_GRP
    count = CELLS_DEV
    slots = 6 * count
    width = NODES * NODES
    span = slots + 4 * GHOST
    device_rows = jnp.arange(devices, dtype=jnp.int32)[:, None]
    traces = face_traces(field.reshape(NODES, NODES, NODES, devices, count)).reshape(width, devices * slots)
    send_index = (send_slots.reshape(devices, 4 * GHOST) + device_rows * slots).reshape(-1).astype(jnp.int32)
    sent = jnp.take(traces, send_index, axis=1).reshape(width, devices, 4, GHOST)
    arrived = [shift_devices(sent[:, :, position], offset) for position, offset in enumerate(curve_offsets)]
    ghosts = jnp.stack(arrived, axis=2).reshape(width, devices, 4 * GHOST)
    pool = jnp.concatenate([traces.reshape(width, devices, slots), ghosts], axis=2).reshape(width, devices * span)
    own_index = (own_slot.reshape(devices, -1) + device_rows * span).reshape(-1).astype(jnp.int32)
    near_index = (near_slot.reshape(devices, -1) + device_rows * span).reshape(-1).astype(jnp.int32)
    own_values = jnp.take(pool, own_index, axis=1).reshape(NODES, NODES, -1)
    near_values = jnp.take(pool, near_index, axis=1).reshape(NODES, NODES, -1)
    own_term, near_term = face_terms(own_values, near_values, kinds, orients, penalty, maps, tables[1])
    gathered = jnp.zeros_like(pool).at[:, own_index].add(own_term.reshape(width, -1))
    gathered = gathered.at[:, near_index].add(near_term.reshape(width, -1))
    gathered = gathered.reshape(width, devices, span)
    local = gathered[:, :, :slots].reshape(width, devices * slots)
    returned = gathered[:, :, slots:].reshape(width, devices, 4, GHOST)
    came_back = [shift_devices(returned[:, :, position], -offset) for position, offset in enumerate(curve_offsets)]
    back = jnp.stack(came_back, axis=2).reshape(width, devices * 4 * GHOST)
    local = local.at[:, send_index].add(back)
    faces = local.reshape(NODES, NODES, devices, 6, count)
    lifted = lift_faces(faces).reshape(NODES, NODES, NODES, devices * count)
    return volume_term(field, scale, tables) + lifted

def reference(right_side, cell_level, own_slot, near_slot, face_kind, orientation, penalty, send_slots, subface_maps):
    tables = node_tables()
    scale = jnp.exp2(-cell_level.astype(jnp.float32))
    devices = N_SFC * N_GRP
    device_rows = jnp.arange(devices, dtype=jnp.int32)[:, None]
    cell_index = (own_slot.reshape(devices, -1) % CELLS_DEV + device_rows * CELLS_DEV).reshape(-1).astype(jnp.int32)
    scaled_penalty = penalty * jnp.take(scale, cell_index)
    solution = jnp.zeros_like(right_side)
    residual = right_side
    direction = right_side
    norm_now = jnp.sum(residual * residual)
    for iteration in range(ITERS):
        image = apply_operator(direction, scale, own_slot, near_slot, face_kind, orientation, scaled_penalty, send_slots, subface_maps, tables)
        step_size = norm_now / jnp.sum(direction * image)
        solution = solution + step_size * direction
        residual = residual - step_size * image
        norm_next = jnp.sum(residual * residual)
        direction = residual + norm_next / norm_now * direction
        norm_now = norm_next
    return (solution, residual)
```

```python
import functools

import jax
import jax.numpy as jnp
import numpy as np
from jax import lax
from jax.experimental import pallas as pl
from jax.experimental.pallas import tpu as pltpu
from jax.sharding import PartitionSpec as P

NODES = 5
WIDTH = NODES * NODES
ROWS = 32
CUBE = 128
ITERS = 3
OFFSETS = (1, -1, 2, -2)
MASS = 1.0
MESH = pl.DeviceIdType.MESH
F32 = jnp.float32
BF16 = jnp.bfloat16


def node_tables():
    points = np.array([-1.0, -np.sqrt(3.0 / 7.0), 0.0, np.sqrt(3.0 / 7.0), 1.0])
    weights = np.array([0.1, 49.0 / 90.0, 32.0 / 45.0, 49.0 / 90.0, 0.1])
    identity = np.eye(5)
    spacing = points[:, None] - points[None, :] + identity
    barycentric = 1.0 / np.prod(spacing, axis=1)
    offdiag = barycentric[None, :] / barycentric[:, None] / spacing
    diagonal = np.sum(1.0 / spacing, axis=1) - 1.0
    derivs = np.where(identity > 0.5, diagonal[:, None], offdiag)
    return derivs.T @ (weights[:, None] * derivs), weights


def constants():
    stiff, w = node_tables()
    mass = np.diag(w)
    kron = lambda a, b, c: np.kron(np.kron(a, b), c)
    volume = np.zeros((CUBE, CUBE))
    volume[:125, :125] = kron(stiff, mass, mass) + kron(mass, stiff, mass) + kron(mass, mass, stiff)
    high = volume.astype(jnp.bfloat16)
    low = (volume - high.astype(np.float64)).astype(jnp.bfloat16)
    volume = np.concatenate([high, high, low], axis=1)
    nodes = np.arange(125).reshape(5, 5, 5)
    layers = [nodes[0], nodes[4], nodes[:, 0], nodes[:, 4], nodes[:, :, 0], nodes[:, :, 4]]
    select = np.zeros((6 * ROWS, CUBE))
    for face, layer in enumerate(layers):
        select[face * ROWS + np.arange(WIDTH), layer.reshape(-1)] = 1.0
    lift = np.concatenate([select.T, select.T], axis=1)
    turn = np.zeros((8, ROWS, ROWS))
    for code in range(8):
        order = np.arange(WIDTH).reshape(5, 5)
        order = order[::-1] if code & 1 else order
        order = order[:, ::-1] if code & 2 else order
        order = order.T if code & 4 else order
        turn[code, np.arange(WIDTH), order.reshape(-1)] = 1.0
    back = np.swapaxes(turn, 1, 2)
    turns = [np.concatenate([m, m], axis=2).reshape(8 * ROWS, 2 * ROWS) for m in (turn, back)]
    face_mass = np.zeros((ROWS, 128))
    face_mass[:WIDTH] = np.outer(w, w).reshape(-1, 1)
    cube_mass = np.zeros((CUBE, 128))
    cube_mass[:125] = MASS * np.einsum("a,b,c->abc", w, w, w).reshape(-1, 1)
    bf = lambda a: jnp.asarray(np.asarray(a, np.float32), BF16)
    return (
        bf(volume),
        bf(select),
        bf(lift),
        bf(turns[0]),
        bf(turns[1]),
        jnp.asarray(np.concatenate([face_mass, cube_mass]), F32),
    )


def split(x):
    high = x.astype(BF16)
    return high, (x - high.astype(F32)).astype(BF16)


def dot(a, b):
    return jnp.dot(a, b, preferred_element_type=F32)


def dot_nt(a, b):
    return lax.dot_general(a, b, (((1,), (1,)), ((), ())), preferred_element_type=F32)


def ring_levels(total):
    levels, stride = [], 1
    while stride < total:
        rest = total // stride
        size = max(g for g in range(1, 33) if rest % g == 0)
        size = rest if size == 1 else size
        levels.append((stride, size))
        stride *= size
    return levels


def kernel(
    dims,
    rhs_ref, level_ref, own_ref, near_ref, kind_ref, orient_ref, pen_ref, send_ref, maps_ref,
    vol_ref, sel_ref, lift_ref, turn_ref, back_ref, mass_ref,
    x_out, r_out,
    field, gather, mapz, diag, psrc, pbuf, xsrc, xbuf, asrc, *rest,
):
    n_sfc, n_grp, count, ghost, pad = dims
    total = n_sfc * n_grp
    levels = ring_levels(total)
    slots_refs = rest[: len(levels)]
    psend, precv, xsend, xrecv, asend, arecv = rest[len(levels):]
    me = lax.axis_index("sfc") * n_grp + lax.axis_index("grp")
    slots = 6 * count
    entries = 4 * ghost
    cols = 4 * pad

    def place(device):
        return (device // n_grp, lax.rem(device, n_grp))

    def near_device(k):
        return place(lax.rem(me + OFFSETS[k] + total, total))

    def peer(level, step):
        stride, size = levels[level]
        digit = lax.rem(me // stride, size)
        return place(me + (lax.rem(digit + step, size) - digit) * stride)

    barrier = pltpu.get_barrier_semaphore()
    greeted = 0
    for level, (_, size) in enumerate(levels):
        def greet(step, carry, level=level):
            pl.semaphore_signal(barrier, inc=1, device_id=peer(level, step), device_id_type=MESH)
            return carry
        lax.fori_loop(1, size, greet, 0)
        greeted += size - 1
    if len(levels) > 1:
        for k in range(4):
            pl.semaphore_signal(barrier, inc=1, device_id=near_device(k), device_id_type=MESH)
        greeted += 4

    own = own_ref[...]
    high_slot = (own >> 8).astype(F32)
    low_slot = (own & 255).astype(F32)
    pen = pen_ref[...]
    pen_a = pen.astype(BF16).astype(F32)
    pen_b = (pen - pen_a).astype(BF16).astype(F32)
    pen_c = pen - pen_a - pen_b
    send = send_ref[...]
    zero_row = jnp.zeros_like(pen)
    params = jnp.concatenate(
        [high_slot, low_slot, kind_ref[...].astype(F32), orient_ref[...].astype(F32), pen_a, pen_b, pen_c, zero_row],
        axis=0,
    ).astype(BF16)
    sent_rows = jnp.concatenate(
        [(send >> 8).astype(F32), (send & 255).astype(F32)] + [zero_row] * 6, axis=0
    ).astype(BF16)
    near = jnp.broadcast_to(near_ref[...], (pad, entries))
    spot = lax.broadcasted_iota(jnp.int32, (pad, entries), 0)
    lane = lax.broadcasted_iota(jnp.int32, (pad, entries), 1)
    inside = spot < ghost
    order, spread = [], []
    for k in range(4):
        order.append(jnp.where(inside & (near == spot + (slots + k * ghost)), 1.0, 0.0).astype(BF16))
        spread.append(jnp.where(inside & (lane == spot + k * ghost), 1.0, 0.0).astype(BF16))
    ordered = dot_nt(params, jnp.concatenate(order, axis=0))
    spread = dot_nt(sent_rows, jnp.concatenate(spread, axis=0))
    own_slot = (ordered[0:1] * 256.0 + ordered[1:2]).astype(jnp.int32)
    send_slot = (spread[0:1] * 256.0 + spread[1:2]).astype(jnp.int32)
    slot_row = lax.broadcasted_iota(jnp.int32, (slots, cols), 0)
    gather[:, cols:] = jnp.where(slot_row == own_slot, 1.0, 0.0).astype(BF16)
    scale = jnp.exp2(-level_ref[...].astype(F32))
    scale_all = jnp.concatenate([jnp.broadcast_to(scale, (8, count))] * 6, axis=1).astype(BF16)
    own_scale = dot(scale_all, gather[:, cols:])[0:1]
    strength = (ordered[4:5] + ordered[5:6] + ordered[6:7]) * own_scale
    sub = lax.broadcasted_iota(jnp.int32, (8, cols), 0)
    tile = jnp.where(sub == 0, ordered[2:3], jnp.where(sub == 1, ordered[3:4], jnp.where(sub == 2, strength, 0.0)))
    for k in range(4):
        psrc[k] = tile[:, k * pad : (k + 1) * pad]

    pl.semaphore_wait(barrier, greeted)

    pcopies = []
    for k in range(4):
        pcopies.append(pltpu.make_async_remote_copy(
            src_ref=psrc.at[k], dst_ref=pbuf.at[k], send_sem=psend.at[k], recv_sem=precv.at[k],
            device_id=near_device(k ^ 1), device_id_type=MESH,
        ))
        pcopies[-1].start()

    gather[:, :cols] = jnp.where(slot_row == send_slot, 1.0, 0.0).astype(BF16)
    mapz[...] = jnp.zeros_like(mapz)
    for s in range(4):
        mapz[s * ROWS : s * ROWS + WIDTH, 0:WIDTH] = maps_ref[s]
    maps = mapz[...]
    map_high, map_low = split(maps[:, :ROWS])
    back_high, back_low = split(maps.T[:ROWS])
    back_twice = jnp.concatenate([back_high, back_high], axis=1)
    face_mass = jnp.concatenate([mass_ref[:ROWS]] * (cols // 128), axis=1)
    cube_mass = mass_ref[ROWS:]
    valid = [
        jnp.where((me + offset >= 0) & (me + offset < total), 1.0, 0.0).astype(F32) for offset in OFFSETS
    ]
    mass_scale = cube_mass * (scale * scale * scale)
    field[...] = jnp.zeros_like(field)
    for g in range(WIDTH):
        field[g * NODES : (g + 1) * NODES] = rhs_ref[g]
    right = field[...]

    def traces(v_high, v_low):
        both = dot(sel_ref[...], jnp.concatenate([v_high, v_low], axis=1))
        rows = [both[f * ROWS : (f + 1) * ROWS] for f in range(6)]
        return jnp.concatenate(
            [
                jnp.concatenate([row[:, :count] for row in rows], axis=1),
                jnp.concatenate([row[:, count:] for row in rows], axis=1),
            ],
            axis=0,
        ).astype(BF16)

    near_info = []
    xcopies = []

    def turned(values, codes, table):
        high, low = split(values)
        forms = dot(table[...], jnp.concatenate([high, low], axis=0))
        result = forms[:ROWS]
        for code in range(1, 8):
            result = jnp.where(codes == code, forms[code * ROWS : (code + 1) * ROWS], result)
        return result

    def operator(v, turn_number):
        v_high, v_low = split(v)
        picked = dot(traces(v_high, v_low), gather[...])
        picked = picked[:ROWS] + picked[ROWS:]
        own_side = picked[:, cols:]
        if not near_info:
            for copy in pcopies:
                copy.wait_recv()
            info = jnp.concatenate([pbuf[k] for k in range(4)], axis=1)
            near_info.append(info[0:1].astype(jnp.int32))
            near_info.append(info[1:2].astype(jnp.int32))
            power = jnp.concatenate([pbuf[k][2:3] * valid[k] for k in range(4)], axis=1)
            diag[:, :cols] = face_mass * power
            diag[:, cols:] = face_mass * strength
        kinds, codes = near_info
        oriented = turned(picked[:, :cols], codes, turn_ref)
        high, low = split(oriented)
        forms = dot(map_high, high) + dot(map_high, low) + dot(map_low, high)
        near_side = jnp.where(kinds == 1, oriented, 0.0)
        for s in range(4):
            near_side = jnp.where(kinds == s + 2, forms[s * ROWS : (s + 1) * ROWS], near_side)
        for k in range(4):
            xsrc[turn_number, k, :, :pad] = near_side[:, k * pad : (k + 1) * pad]
            xsrc[turn_number, k, :, pad:] = own_side[:, (k ^ 1) * pad : ((k ^ 1) + 1) * pad]
        copies = []
        for k in range(4):
            copies.append(pltpu.make_async_remote_copy(
                src_ref=xsrc.at[turn_number, k], dst_ref=xbuf.at[turn_number, k ^ 1],
                send_sem=xsend.at[turn_number, k], recv_sem=xrecv.at[turn_number, k ^ 1],
                device_id=near_device(k), device_id_type=MESH,
            ))
            copies[-1].start()
        xcopies.extend(copies)
        image = dot(vol_ref[:, : 2 * CUBE], jnp.concatenate([v_high, v_low], axis=0))
        image = (image + dot(vol_ref[:, 2 * CUBE :], v_high)) * scale + mass_scale * v
        for copy in copies:
            copy.wait_recv()
        near_got = jnp.concatenate([xbuf[turn_number, k, :, pad:] for k in range(4)], axis=1)
        own_got = jnp.concatenate([xbuf[turn_number, k ^ 1, :, :pad] * valid[k ^ 1] for k in range(4)], axis=1)
        near_flux = diag[:, :cols] * (near_side - near_got)
        own_flux = diag[:, cols:] * (own_side - own_got)
        stacked = jnp.concatenate([jnp.where(kinds == s + 2, near_flux, 0.0) for s in range(4)], axis=0)
        high, low = split(stacked)
        near_flux = jnp.where(kinds == 1, near_flux, 0.0)
        near_flux = near_flux + dot(back_twice, jnp.concatenate([high, low], axis=0)) + dot(back_low, high)
        near_flux = turned(near_flux, codes, back_ref)
        flux = jnp.concatenate([near_flux, own_flux], axis=1)
        faces = dot_nt(jnp.concatenate(split(flux), axis=0), gather[...])
        faces = faces[:ROWS] + faces[ROWS:]
        faces = jnp.concatenate([faces[:, f * count : (f + 1) * count] for f in range(6)], axis=0)
        return image + dot(lift_ref[...], jnp.concatenate(split(faces), axis=0))

    def level_copy(turn_number, level, step):
        return pltpu.make_async_remote_copy(
            src_ref=asrc.at[turn_number, level], dst_ref=slots_refs[level].at[turn_number, step - 1],
            send_sem=asend.at[turn_number, level], recv_sem=arecv.at[turn_number, level],
            device_id=peer(level, step), device_id_type=MESH,
        )

    def level_start(turn_number, level):
        def start(step, carry):
            level_copy(turn_number, level, step).start()
            return carry
        lax.fori_loop(1, levels[level][1], start, 0)

    def sums_start(turn_number, pairs):
        for i, (a, b) in enumerate(pairs):
            asrc[turn_number, 0, i : i + 1, :] = jnp.sum(a * b, axis=0, keepdims=True)
        level_start(turn_number, 0)

    def sums_wait(turn_number, number):
        for level in range(len(levels)):
            landed = slots_refs[level].at[turn_number]
            pltpu.make_async_copy(landed, landed, arecv.at[turn_number, level]).wait()
            value = asrc[turn_number, level] + jnp.sum(landed[...], axis=0)
            if level + 1 < len(levels):
                asrc[turn_number, level + 1] = value
                level_start(turn_number, level + 1)
        value = jnp.broadcast_to(jnp.sum(value, axis=1, keepdims=True), (8, 128))
        return [value[i : i + 1] for i in range(number)]

    asrc[...] = jnp.zeros_like(asrc)
    r = right
    w = operator(r, 0)
    x = p = s = z = None
    norm_last = None
    for it in range(ITERS):
        pairs = [(r, r), (r, w)]
        if it:
            pairs += [(r, s), (p, w), (p, s)]
        sums_start(it, pairs)
        q = operator(w, it + 1) if it + 1 < ITERS else None
        sums = sums_wait(it, len(pairs))
        norm = sums[0]
        if it == 0:
            alpha = norm / sums[1]
            p, s, z = r, w, q
            x = alpha * p
        else:
            beta = norm / norm_last
            alpha = norm / (sums[1] + beta * (sums[2] + sums[3]) + beta * beta * sums[4])
            p = r + beta * p
            s = w + beta * s
            x = x + alpha * p
            if q is not None:
                z = q + beta * z
        r = r - alpha * s
        if q is not None:
            w = w - alpha * z
        norm_last = norm

    field[...] = x
    for g in range(WIDTH):
        x_out[g] = field[g * NODES : (g + 1) * NODES]
    mapz[...] = r
    for g in range(WIDTH):
        r_out[g] = mapz[g * NODES : (g + 1) * NODES]

    for copy in pcopies + xcopies:
        copy.wait_send()
    for it in range(ITERS):
        for level in range(len(levels)):
            landed = slots_refs[level].at[it]
            pltpu.make_async_copy(landed, landed, asend.at[it, level]).wait()


def body(n_sfc, n_grp, right_side, cell_level, own_slot, near_slot, face_kind, orientation, penalty, send_slots, maps):
    count = right_side.shape[-1]
    ghost = send_slots.shape[0] // 4
    pad = -(-ghost // 128) * 128
    levels = ring_levels(n_sfc * n_grp)
    row = lambda a: a.reshape(1, -1)
    vmem = pl.BlockSpec(memory_space=pltpu.VMEM)
    dma = pltpu.SemaphoreType.DMA
    shape = jax.ShapeDtypeStruct((WIDTH, NODES, count), F32)
    x, r = pl.pallas_call(
        functools.partial(kernel, (n_sfc, n_grp, count, ghost, pad)),
        out_shape=(shape, shape),
        in_specs=[vmem] * 15,
        out_specs=(vmem, vmem),
        scratch_shapes=[
            pltpu.VMEM((CUBE, count), F32),
            pltpu.VMEM((6 * count, 8 * pad), BF16),
            pltpu.VMEM((4 * ROWS, 128), F32),
            pltpu.VMEM((ROWS, 8 * pad), F32),
            pltpu.VMEM((4, 8, pad), F32),
            pltpu.VMEM((4, 8, pad), F32),
            pltpu.VMEM((ITERS, 4, ROWS, 2 * pad), F32),
            pltpu.VMEM((ITERS, 4, ROWS, 2 * pad), F32),
            pltpu.VMEM((ITERS, len(levels), 8, 128), F32),
        ]
        + [pltpu.VMEM((ITERS, size - 1, 8, 128), F32) for _, size in levels]
        + [
            dma((4,)),
            dma((4,)),
            dma((ITERS, 4)),
            dma((ITERS, 4)),
            dma((ITERS, len(levels))),
            dma((ITERS, len(levels))),
        ],
        compiler_params=pltpu.CompilerParams(collective_id=0, has_side_effects=True),
    )(
        right_side.reshape(WIDTH, NODES, count),
        row(cell_level), row(own_slot), row(near_slot), row(face_kind), row(orientation), row(penalty), row(send_slots),
        maps, *constants(),
    )
    return x.reshape(right_side.shape), r.reshape(right_side.shape)


def solution(mesh):
    split_spec = P(("sfc", "grp"))
    field_spec = P(None, None, None, ("sfc", "grp"))
    return jax.shard_map(
        functools.partial(body, mesh.shape["sfc"], mesh.shape["grp"]),
        mesh=mesh,
        in_specs=(field_spec,) + (split_spec,) * 7 + (P(),),
        out_specs=(field_spec, field_spec),
        check_vma=False,
    )
```

```python
import functools

import jax
import jax.numpy as jnp
import numpy as np
from jax import lax
from jax.experimental import pallas as pl
from jax.experimental.pallas import tpu as pltpu
from jax.sharding import PartitionSpec as P

NODES = 5
WIDTH = NODES * NODES
ROWS = 32
CUBE = 128
ITERS = 3
OFFSETS = (1, -1, 2, -2)
MASS = 1.0
MESH = pl.DeviceIdType.MESH
F32 = jnp.float32
BF16 = jnp.bfloat16


def node_tables():
    points = np.array([-1.0, -np.sqrt(3.0 / 7.0), 0.0, np.sqrt(3.0 / 7.0), 1.0])
    weights = np.array([0.1, 49.0 / 90.0, 32.0 / 45.0, 49.0 / 90.0, 0.1])
    identity = np.eye(5)
    spacing = points[:, None] - points[None, :] + identity
    barycentric = 1.0 / np.prod(spacing, axis=1)
    offdiag = barycentric[None, :] / barycentric[:, None] / spacing
    diagonal = np.sum(1.0 / spacing, axis=1) - 1.0
    derivs = np.where(identity > 0.5, diagonal[:, None], offdiag)
    return derivs.T @ (weights[:, None] * derivs), weights


def constants():
    stiff, w = node_tables()
    mass = np.diag(w)
    kron = lambda a, b, c: np.kron(np.kron(a, b), c)
    volume = np.zeros((CUBE, CUBE))
    volume[:125, :125] = kron(stiff, mass, mass) + kron(mass, stiff, mass) + kron(mass, mass, stiff)
    high = volume.astype(jnp.bfloat16)
    low = (volume - high.astype(np.float64)).astype(jnp.bfloat16)
    volume = np.concatenate([high, high, low], axis=1)
    nodes = np.arange(125).reshape(5, 5, 5)
    layers = [nodes[0], nodes[4], nodes[:, 0], nodes[:, 4], nodes[:, :, 0], nodes[:, :, 4]]
    select = np.zeros((6 * ROWS, CUBE))
    for face, layer in enumerate(layers):
        select[face * ROWS + np.arange(WIDTH), layer.reshape(-1)] = 1.0
    lift = np.concatenate([select.T, select.T], axis=1)
    turn = np.zeros((8, ROWS, ROWS))
    for code in range(8):
        order = np.arange(WIDTH).reshape(5, 5)
        order = order[::-1] if code & 1 else order
        order = order[:, ::-1] if code & 2 else order
        order = order.T if code & 4 else order
        turn[code, np.arange(WIDTH), order.reshape(-1)] = 1.0
    back = np.swapaxes(turn, 1, 2)
    turns = [np.concatenate([m, m], axis=2).reshape(8 * ROWS, 2 * ROWS) for m in (turn, back)]
    face_mass = np.zeros((ROWS, 128))
    face_mass[:WIDTH] = np.outer(w, w).reshape(-1, 1)
    cube_mass = np.zeros((CUBE, 128))
    cube_mass[:125] = MASS * np.einsum("a,b,c->abc", w, w, w).reshape(-1, 1)
    bf = lambda a: jnp.asarray(np.asarray(a, np.float32), BF16)
    return (
        bf(volume),
        bf(select),
        bf(lift),
        bf(turns[0]),
        bf(turns[1]),
        jnp.asarray(np.concatenate([face_mass, cube_mass]), F32),
    )


def split(x):
    high = x.astype(BF16)
    return high, (x - high.astype(F32)).astype(BF16)


def dot(a, b):
    return jnp.dot(a, b, preferred_element_type=F32)


def dot_nt(a, b):
    return lax.dot_general(a, b, (((1,), (1,)), ((), ())), preferred_element_type=F32)


def ring_levels(total):
    levels, stride = [], 1
    while stride < total:
        rest = total // stride
        size = max(g for g in range(1, 33) if rest % g == 0)
        size = rest if size == 1 else size
        levels.append((stride, size))
        stride *= size
    return levels


def kernel(
    dims,
    rhs_ref, level_ref, own_ref, near_ref, kind_ref, orient_ref, pen_ref, send_ref, maps_ref,
    vol_ref, sel_ref, lift_ref, turn_ref, back_ref, mass_ref,
    x_out, r_out,
    field, gather, mapz, diag, psrc, pbuf, xsrc, xbuf, asrc, *rest,
):
    n_sfc, n_grp, count, ghost, pad = dims
    total = n_sfc * n_grp
    levels = ring_levels(total)
    slots_refs = rest[: len(levels)]
    psend, precv, xsend, xrecv, asend, arecv = rest[len(levels):]
    me = lax.axis_index("sfc") * n_grp + lax.axis_index("grp")
    slots = 6 * count
    entries = 4 * ghost
    cols = 4 * pad

    def place(device):
        return (device // n_grp, lax.rem(device, n_grp))

    def near_device(k):
        return place(lax.rem(me + OFFSETS[k] + total, total))

    def peer(level, step):
        stride, size = levels[level]
        digit = lax.rem(me // stride, size)
        return place(me + (lax.rem(digit + step, size) - digit) * stride)

    exists = [(me + offset >= 0) & (me + offset < total) for offset in OFFSETS]

    def guarded(k, action):
        @pl.when(exists[k])
        def _():
            action()

    for k in range(4):
        @pl.when(jnp.logical_not(exists[k]))
        def _(k=k):
            pbuf[k] = jnp.zeros((8, pad), F32)
            for it in range(ITERS):
                xbuf[it, k] = jnp.zeros((ROWS, 2 * pad), F32)

    barrier = pltpu.get_barrier_semaphore()
    greeted = 0
    for level, (_, size) in enumerate(levels):
        def greet(step, carry, level=level):
            pl.semaphore_signal(barrier, inc=1, device_id=peer(level, step), device_id_type=MESH)
            return carry
        lax.fori_loop(1, size, greet, 0)
        greeted += size - 1
    if len(levels) > 1:
        for k in range(4):
            pl.semaphore_signal(barrier, inc=1, device_id=near_device(k), device_id_type=MESH)
        greeted += 4

    line = lambda ref: ref[...].reshape(1, -1)
    own = line(own_ref)
    high_slot = (own >> 8).astype(F32)
    low_slot = (own & 255).astype(F32)
    pen = line(pen_ref)
    pen_a = pen.astype(BF16).astype(F32)
    pen_b = (pen - pen_a).astype(BF16).astype(F32)
    pen_c = pen - pen_a - pen_b
    send = line(send_ref)
    zero_row = jnp.zeros_like(pen)
    params = jnp.concatenate(
        [high_slot, low_slot, line(kind_ref).astype(F32), line(orient_ref).astype(F32), pen_a, pen_b, pen_c, zero_row],
        axis=0,
    ).astype(BF16)
    sent_rows = jnp.concatenate(
        [(send >> 8).astype(F32), (send & 255).astype(F32)] + [zero_row] * 6, axis=0
    ).astype(BF16)
    near = jnp.broadcast_to(line(near_ref), (pad, entries))
    spot = lax.broadcasted_iota(jnp.int32, (pad, entries), 0)
    lane = lax.broadcasted_iota(jnp.int32, (pad, entries), 1)
    inside = spot < ghost
    order, spread = [], []
    for k in range(4):
        order.append(jnp.where(inside & (near == spot + (slots + k * ghost)), 1.0, 0.0).astype(BF16))
        spread.append(jnp.where(inside & (lane == spot + k * ghost), 1.0, 0.0).astype(BF16))
    ordered = dot_nt(params, jnp.concatenate(order, axis=0))
    spread = dot_nt(sent_rows, jnp.concatenate(spread, axis=0))
    own_slot = (ordered[0:1] * 256.0 + ordered[1:2]).astype(jnp.int32)
    send_slot = (spread[0:1] * 256.0 + spread[1:2]).astype(jnp.int32)
    slot_row = lax.broadcasted_iota(jnp.int32, (slots, cols), 0)
    gather[:, cols:] = jnp.where(slot_row == own_slot, 1.0, 0.0).astype(BF16)
    scale = jnp.exp2(-line(level_ref).astype(F32))
    scale_all = jnp.concatenate([jnp.broadcast_to(scale, (8, count))] * 6, axis=1).astype(BF16)
    own_scale = dot(scale_all, gather[:, cols:])[0:1]
    strength = (ordered[4:5] + ordered[5:6] + ordered[6:7]) * own_scale
    sub = lax.broadcasted_iota(jnp.int32, (8, cols), 0)
    tile = jnp.where(sub == 0, ordered[2:3], jnp.where(sub == 1, ordered[3:4], jnp.where(sub == 2, strength, 0.0)))
    for k in range(4):
        psrc[k] = tile[:, k * pad : (k + 1) * pad]

    pl.semaphore_wait(barrier, greeted)

    pcopies = []
    for k in range(4):
        pcopies.append(pltpu.make_async_remote_copy(
            src_ref=psrc.at[k], dst_ref=pbuf.at[k], send_sem=psend.at[k], recv_sem=precv.at[k],
            device_id=near_device(k ^ 1), device_id_type=MESH,
        ))
        guarded(k ^ 1, pcopies[-1].start)

    gather[:, :cols] = jnp.where(slot_row == send_slot, 1.0, 0.0).astype(BF16)
    mapz[...] = jnp.zeros_like(mapz)
    for s in range(4):
        mapz[s * ROWS : s * ROWS + WIDTH, 0:WIDTH] = maps_ref[:, s, :]
    maps = mapz[...]
    map_high, map_low = split(maps[:, :ROWS])
    back_high, back_low = split(maps.T[:ROWS])
    back_twice = jnp.concatenate([back_high, back_high], axis=1)
    face_mass = jnp.concatenate([mass_ref[:ROWS]] * (cols // 128), axis=1)
    cube_mass = mass_ref[ROWS:]
    mass_scale = cube_mass * (scale * scale * scale)
    field[...] = jnp.zeros_like(field)
    for g in range(WIDTH):
        field[g * NODES : (g + 1) * NODES] = rhs_ref[g]
    right = field[...]

    def traces(v_high, v_low):
        both = dot(sel_ref[...], jnp.concatenate([v_high, v_low], axis=1))
        rows = [both[f * ROWS : (f + 1) * ROWS] for f in range(6)]
        return jnp.concatenate(
            [
                jnp.concatenate([row[:, :count] for row in rows], axis=1),
                jnp.concatenate([row[:, count:] for row in rows], axis=1),
            ],
            axis=0,
        ).astype(BF16)

    near_info = []
    xcopies = []

    def turned(values, codes, table):
        high, low = split(values)
        forms = dot(table[...], jnp.concatenate([high, low], axis=0))
        result = forms[:ROWS]
        for code in range(1, 8):
            result = jnp.where(codes == code, forms[code * ROWS : (code + 1) * ROWS], result)
        return result

    def operator(v, turn_number):
        v_high, v_low = split(v)
        picked = dot(traces(v_high, v_low), gather[...])
        picked = picked[:ROWS] + picked[ROWS:]
        own_side = picked[:, cols:]
        if not near_info:
            for k in range(4):
                guarded(k, pcopies[k].wait_recv)
            info = jnp.concatenate([pbuf[k] for k in range(4)], axis=1)
            near_info.append(info[0:1].astype(jnp.int32))
            near_info.append(info[1:2].astype(jnp.int32))
            power = jnp.concatenate([pbuf[k][2:3] for k in range(4)], axis=1)
            diag[:, :cols] = face_mass * power
            diag[:, cols:] = face_mass * strength
        kinds, codes = near_info
        oriented = turned(picked[:, :cols], codes, turn_ref)
        high, low = split(oriented)
        forms = dot(map_high, high) + dot(map_high, low) + dot(map_low, high)
        near_side = jnp.where(kinds == 1, oriented, 0.0)
        for s in range(4):
            near_side = jnp.where(kinds == s + 2, forms[s * ROWS : (s + 1) * ROWS], near_side)
        for k in range(4):
            xsrc[turn_number, k, :, :pad] = near_side[:, k * pad : (k + 1) * pad]
            xsrc[turn_number, k, :, pad:] = own_side[:, (k ^ 1) * pad : ((k ^ 1) + 1) * pad]
        copies = []
        for k in range(4):
            copies.append(pltpu.make_async_remote_copy(
                src_ref=xsrc.at[turn_number, k], dst_ref=xbuf.at[turn_number, k ^ 1],
                send_sem=xsend.at[turn_number, k], recv_sem=xrecv.at[turn_number, k ^ 1],
                device_id=near_device(k), device_id_type=MESH,
            ))
            guarded(k, copies[-1].start)
        xcopies.append(copies)
        image = dot(vol_ref[:, : 2 * CUBE], jnp.concatenate([v_high, v_low], axis=0))
        image = (image + dot(vol_ref[:, 2 * CUBE :], v_high)) * scale + mass_scale * v
        for k in range(4):
            guarded(k ^ 1, copies[k].wait_recv)
        near_got = jnp.concatenate([xbuf[turn_number, k, :, pad:] for k in range(4)], axis=1)
        own_got = jnp.concatenate([xbuf[turn_number, k ^ 1, :, :pad] for k in range(4)], axis=1)
        near_flux = diag[:, :cols] * (near_side - near_got)
        own_flux = diag[:, cols:] * (own_side - own_got)
        stacked = jnp.concatenate([jnp.where(kinds == s + 2, near_flux, 0.0) for s in range(4)], axis=0)
        high, low = split(stacked)
        near_flux = jnp.where(kinds == 1, near_flux, 0.0)
        near_flux = near_flux + dot(back_twice, jnp.concatenate([high, low], axis=0)) + dot(back_low, high)
        near_flux = turned(near_flux, codes, back_ref)
        flux = jnp.concatenate([near_flux, own_flux], axis=1)
        faces = dot_nt(jnp.concatenate(split(flux), axis=0), gather[...])
        faces = faces[:ROWS] + faces[ROWS:]
        faces = jnp.concatenate([faces[:, f * count : (f + 1) * count] for f in range(6)], axis=0)
        return image + dot(lift_ref[...], jnp.concatenate(split(faces), axis=0))

    def level_copy(turn_number, level, step):
        return pltpu.make_async_remote_copy(
            src_ref=asrc.at[turn_number, level], dst_ref=slots_refs[level].at[turn_number, step - 1],
            send_sem=asend.at[turn_number, level], recv_sem=arecv.at[turn_number, level],
            device_id=peer(level, step), device_id_type=MESH,
        )

    def level_start(turn_number, level):
        def start(step, carry):
            level_copy(turn_number, level, step).start()
            return carry
        lax.fori_loop(1, levels[level][1], start, 0)

    def sums_start(turn_number, pairs):
        for i, (a, b) in enumerate(pairs):
            asrc[turn_number, 0, i : i + 1, :] = jnp.sum(a * b, axis=0, keepdims=True)
        level_start(turn_number, 0)

    def sums_wait(turn_number, number):
        for level in range(len(levels)):
            landed = slots_refs[level].at[turn_number]
            pltpu.make_async_copy(landed, landed, arecv.at[turn_number, level]).wait()
            value = asrc[turn_number, level] + jnp.sum(landed[...], axis=0)
            if level + 1 < len(levels):
                asrc[turn_number, level + 1] = value
                level_start(turn_number, level + 1)
        value = jnp.broadcast_to(jnp.sum(value, axis=1, keepdims=True), (8, 128))
        return [value[i : i + 1] for i in range(number)]

    asrc[...] = jnp.zeros_like(asrc)
    r = right
    w = operator(r, 0)
    x = p = s = z = None
    norm_last = None
    for it in range(ITERS):
        pairs = [(r, r), (r, w)]
        if it:
            pairs += [(r, s), (p, w), (p, s)]
        sums_start(it, pairs)
        q = operator(w, it + 1) if it + 1 < ITERS else None
        sums = sums_wait(it, len(pairs))
        norm = sums[0]
        if it == 0:
            alpha = norm / sums[1]
            p, s, z = r, w, q
            x = alpha * p
        else:
            beta = norm / norm_last
            alpha = norm / (sums[1] + beta * (sums[2] + sums[3]) + beta * beta * sums[4])
            p = r + beta * p
            s = w + beta * s
            x = x + alpha * p
            if q is not None:
                z = q + beta * z
        r = r - alpha * s
        if q is not None:
            w = w - alpha * z
        norm_last = norm

    field[...] = x
    for g in range(WIDTH):
        x_out[g] = field[g * NODES : (g + 1) * NODES]
    mapz[...] = r
    for g in range(WIDTH):
        r_out[g] = mapz[g * NODES : (g + 1) * NODES]

    for k in range(4):
        guarded(k ^ 1, pcopies[k].wait_send)
        for copies in xcopies:
            guarded(k, copies[k].wait_send)
    for it in range(ITERS):
        for level in range(len(levels)):
            landed = slots_refs[level].at[it]
            pltpu.make_async_copy(landed, landed, asend.at[it, level]).wait()


def body(n_sfc, n_grp, right_side, cell_level, own_slot, near_slot, face_kind, orientation, penalty, send_slots, maps):
    count = right_side.shape[-1]
    ghost = send_slots.shape[0] // 4
    pad = -(-ghost // 128) * 128
    levels = ring_levels(n_sfc * n_grp)
    vmem = pl.BlockSpec(memory_space=pltpu.VMEM)
    dma = pltpu.SemaphoreType.DMA
    shape = jax.ShapeDtypeStruct((WIDTH, NODES, count), F32)
    x, r = pl.pallas_call(
        functools.partial(kernel, (n_sfc, n_grp, count, ghost, pad)),
        out_shape=(shape, shape),
        in_specs=[vmem] * 15,
        out_specs=(vmem, vmem),
        scratch_shapes=[
            pltpu.VMEM((CUBE, count), F32),
            pltpu.VMEM((6 * count, 8 * pad), BF16),
            pltpu.VMEM((4 * ROWS, 128), F32),
            pltpu.VMEM((ROWS, 8 * pad), F32),
            pltpu.VMEM((4, 8, pad), F32),
            pltpu.VMEM((4, 8, pad), F32),
            pltpu.VMEM((ITERS, 4, ROWS, 2 * pad), F32),
            pltpu.VMEM((ITERS, 4, ROWS, 2 * pad), F32),
            pltpu.VMEM((ITERS, len(levels), 8, 128), F32),
        ]
        + [pltpu.VMEM((ITERS, size - 1, 8, 128), F32) for _, size in levels]
        + [
            dma((4,)),
            dma((4,)),
            dma((ITERS, 4)),
            dma((ITERS, 4)),
            dma((ITERS, len(levels))),
            dma((ITERS, len(levels))),
        ],
        compiler_params=pltpu.CompilerParams(collective_id=0, has_side_effects=True),
    )(
        right_side.reshape(WIDTH, NODES, count),
        cell_level, own_slot, near_slot, face_kind, orientation, penalty, send_slots,
        jnp.swapaxes(maps, 0, 1), *constants(),
    )
    return x.reshape(right_side.shape), r.reshape(right_side.shape)


def solution(mesh):
    split_spec = P(("sfc", "grp"))
    field_spec = P(None, None, None, ("sfc", "grp"))
    return jax.shard_map(
        functools.partial(body, mesh.shape["sfc"], mesh.shape["grp"]),
        mesh=mesh,
        in_specs=(field_spec,) + (split_spec,) * 7 + (P(),),
        out_specs=(field_spec, field_spec),
        check_vma=False,
    )
```

```python
import functools

import jax
import jax.numpy as jnp
import numpy as np
from jax import lax
from jax.experimental import pallas as pl
from jax.experimental.pallas import tpu as pltpu
from jax.sharding import PartitionSpec as P

NODES = 5
WIDTH = NODES * NODES
ROWS = 32
CUBE = 128
ITERS = 3
OFFSETS = (1, -1, 2, -2)
MASS = 1.0
MESH = pl.DeviceIdType.MESH
F32 = jnp.float32
BF16 = jnp.bfloat16


def node_tables():
    points = np.array([-1.0, -np.sqrt(3.0 / 7.0), 0.0, np.sqrt(3.0 / 7.0), 1.0])
    weights = np.array([0.1, 49.0 / 90.0, 32.0 / 45.0, 49.0 / 90.0, 0.1])
    identity = np.eye(5)
    spacing = points[:, None] - points[None, :] + identity
    barycentric = 1.0 / np.prod(spacing, axis=1)
    offdiag = barycentric[None, :] / barycentric[:, None] / spacing
    diagonal = np.sum(1.0 / spacing, axis=1) - 1.0
    derivs = np.where(identity > 0.5, diagonal[:, None], offdiag)
    return derivs.T @ (weights[:, None] * derivs), weights


def constants():
    stiff, w = node_tables()
    mass = np.diag(w)
    kron = lambda a, b, c: np.kron(np.kron(a, b), c)
    volume = np.zeros((CUBE, CUBE))
    volume[:125, :125] = kron(stiff, mass, mass) + kron(mass, stiff, mass) + kron(mass, mass, stiff)
    high = volume.astype(jnp.bfloat16)
    low = (volume - high.astype(np.float64)).astype(jnp.bfloat16)
    volume = np.concatenate([high, high, low], axis=1)
    nodes = np.arange(125).reshape(5, 5, 5)
    layers = [nodes[0], nodes[4], nodes[:, 0], nodes[:, 4], nodes[:, :, 0], nodes[:, :, 4]]
    select = np.zeros((6 * ROWS, CUBE))
    for face, layer in enumerate(layers):
        select[face * ROWS + np.arange(WIDTH), layer.reshape(-1)] = 1.0
    lift = np.concatenate([select.T, select.T], axis=1)
    turn = np.zeros((8, ROWS, ROWS))
    for code in range(8):
        order = np.arange(WIDTH).reshape(5, 5)
        order = order[::-1] if code & 1 else order
        order = order[:, ::-1] if code & 2 else order
        order = order.T if code & 4 else order
        turn[code, np.arange(WIDTH), order.reshape(-1)] = 1.0
    back = np.swapaxes(turn, 1, 2)
    turns = [np.concatenate([m, m], axis=2).reshape(8 * ROWS, 2 * ROWS) for m in (turn, back)]
    face_mass = np.zeros((ROWS, 128))
    face_mass[:WIDTH] = np.outer(w, w).reshape(-1, 1)
    cube_mass = np.zeros((CUBE, 128))
    cube_mass[:125] = MASS * np.einsum("a,b,c->abc", w, w, w).reshape(-1, 1)
    bf = lambda a: jnp.asarray(np.asarray(a, np.float32), BF16)
    return (
        bf(volume),
        bf(select),
        bf(lift),
        bf(turns[0]),
        bf(turns[1]),
        jnp.asarray(np.concatenate([face_mass, cube_mass]), F32),
    )


def split(x):
    high = x.astype(BF16)
    return high, (x - high.astype(F32)).astype(BF16)


def dot(a, b):
    return jnp.dot(a, b, preferred_element_type=F32)


def dot_nt(a, b):
    return lax.dot_general(a, b, (((1,), (1,)), ((), ())), preferred_element_type=F32)


def ring_levels(total):
    levels, stride = [], 1
    while stride < total:
        rest = total // stride
        size = max(g for g in range(1, 33) if rest % g == 0)
        size = rest if size == 1 else size
        levels.append((stride, size))
        stride *= size
    return levels


def tail_rows(ghost, pad):
    return ROWS // 2 if pad == 128 and 64 < ghost <= 96 else ROWS


def pack(first, second, ghost, pad):
    if tail_rows(ghost, pad) == ROWS:
        return first, second
    lane = lax.broadcasted_iota(jnp.int32, (ROWS, pad), 1)
    half = ROWS // 2
    moved = pltpu.roll(second, ghost, 1)
    tail = jnp.where(lane[:half] < 64, moved[:half], pltpu.roll(moved[half:], 64, 1))
    return jnp.where(lane < ghost, first, moved), tail


def unpack(main, tail, ghost, pad):
    if tail_rows(ghost, pad) == ROWS:
        return main, tail
    lane = lax.broadcasted_iota(jnp.int32, (ROWS, pad), 1)
    moved = jnp.concatenate([tail, pltpu.roll(tail, 64, 1)], axis=0)
    return main, pltpu.roll(jnp.where(lane < ghost, moved, main), pad - ghost, 1)


def kernel(
    dims,
    rhs_ref, level_ref, own_ref, near_ref, kind_ref, orient_ref, pen_ref, send_ref, maps_ref,
    vol_ref, sel_ref, lift_ref, turn_ref, back_ref, mass_ref,
    x_out, r_out,
    field, gather, mapz, diag, psrc, pbuf, xsrc, xbuf, asrc, *rest,
):
    n_sfc, n_grp, count, ghost, pad = dims
    total = n_sfc * n_grp
    levels = ring_levels(total)
    slots_refs = rest[: len(levels)]
    psend, precv, xsend, xrecv, asend, arecv = rest[len(levels):]
    me = lax.axis_index("sfc") * n_grp + lax.axis_index("grp")
    slots = 6 * count
    entries = 4 * ghost
    cols = 4 * pad

    def place(device):
        return (device // n_grp, lax.rem(device, n_grp))

    def near_device(k):
        return place(lax.rem(me + OFFSETS[k] + total, total))

    def peer(level, step):
        stride, size = levels[level]
        digit = lax.rem(me // stride, size)
        return place(me + (lax.rem(digit + step, size) - digit) * stride)

    exists = [(me + offset >= 0) & (me + offset < total) for offset in OFFSETS]

    def guarded(k, action):
        @pl.when(exists[k])
        def _():
            action()

    for k in range(4):
        @pl.when(jnp.logical_not(exists[k]))
        def _(k=k):
            pbuf[k] = jnp.zeros((8, pad), F32)
            for it in range(ITERS):
                xbuf[it, k] = jnp.zeros(xbuf.shape[2:], F32)

    barrier = pltpu.get_barrier_semaphore()
    greeted = 0
    for level, (_, size) in enumerate(levels):
        def greet(step, carry, level=level):
            pl.semaphore_signal(barrier, inc=1, device_id=peer(level, step), device_id_type=MESH)
            return carry
        lax.fori_loop(1, size, greet, 0)
        greeted += size - 1
    if len(levels) > 1:
        for k in range(4):
            pl.semaphore_signal(barrier, inc=1, device_id=near_device(k), device_id_type=MESH)
        greeted += 4

    line = lambda ref: ref[...].reshape(1, -1)
    own = line(own_ref)
    high_slot = (own >> 8).astype(F32)
    low_slot = (own & 255).astype(F32)
    pen = line(pen_ref)
    pen_a = pen.astype(BF16).astype(F32)
    pen_b = (pen - pen_a).astype(BF16).astype(F32)
    pen_c = pen - pen_a - pen_b
    send = line(send_ref)
    zero_row = jnp.zeros_like(pen)
    params = jnp.concatenate(
        [high_slot, low_slot, line(kind_ref).astype(F32), line(orient_ref).astype(F32), pen_a, pen_b, pen_c, zero_row],
        axis=0,
    ).astype(BF16)
    sent_rows = jnp.concatenate(
        [(send >> 8).astype(F32), (send & 255).astype(F32)] + [zero_row] * 6, axis=0
    ).astype(BF16)
    near = jnp.broadcast_to(line(near_ref), (pad, entries))
    spot = lax.broadcasted_iota(jnp.int32, (pad, entries), 0)
    lane = lax.broadcasted_iota(jnp.int32, (pad, entries), 1)
    inside = spot < ghost
    order, spread = [], []
    for k in range(4):
        order.append(jnp.where(inside & (near == spot + (slots + k * ghost)), 1.0, 0.0).astype(BF16))
        spread.append(jnp.where(inside & (lane == spot + k * ghost), 1.0, 0.0).astype(BF16))
    ordered = dot_nt(params, jnp.concatenate(order, axis=0))
    spread = dot_nt(sent_rows, jnp.concatenate(spread, axis=0))
    own_slot = (ordered[0:1] * 256.0 + ordered[1:2]).astype(jnp.int32)
    send_slot = (spread[0:1] * 256.0 + spread[1:2]).astype(jnp.int32)
    slot_row = lax.broadcasted_iota(jnp.int32, (slots, cols), 0)
    gather[:, cols:] = jnp.where(slot_row == own_slot, 1.0, 0.0).astype(BF16)
    scale = jnp.exp2(-line(level_ref).astype(F32))
    scale_all = jnp.concatenate([jnp.broadcast_to(scale, (8, count))] * 6, axis=1).astype(BF16)
    own_scale = dot(scale_all, gather[:, cols:])[0:1]
    strength = (ordered[4:5] + ordered[5:6] + ordered[6:7]) * own_scale
    sub = lax.broadcasted_iota(jnp.int32, (8, cols), 0)
    tile = jnp.where(sub == 0, ordered[2:3], jnp.where(sub == 1, ordered[3:4], jnp.where(sub == 2, strength, 0.0)))
    for k in range(4):
        psrc[k] = tile[:, k * pad : (k + 1) * pad]

    pl.semaphore_wait(barrier, greeted)

    pcopies = []
    for k in range(4):
        pcopies.append(pltpu.make_async_remote_copy(
            src_ref=psrc.at[k], dst_ref=pbuf.at[k], send_sem=psend.at[k], recv_sem=precv.at[k],
            device_id=near_device(k ^ 1), device_id_type=MESH,
        ))
        guarded(k ^ 1, pcopies[-1].start)

    gather[:, :cols] = jnp.where(slot_row == send_slot, 1.0, 0.0).astype(BF16)
    mapz[...] = jnp.zeros_like(mapz)
    for s in range(4):
        mapz[s * ROWS : s * ROWS + WIDTH, 0:WIDTH] = maps_ref[:, s, :]
    maps = mapz[...]
    map_high, map_low = split(maps[:, :ROWS])
    back_high, back_low = split(maps.T[:ROWS])
    back_twice = jnp.concatenate([back_high, back_high], axis=1)
    face_mass = jnp.concatenate([mass_ref[:ROWS]] * (cols // 128), axis=1)
    cube_mass = mass_ref[ROWS:]
    mass_scale = cube_mass * (scale * scale * scale)
    field[...] = jnp.zeros_like(field)
    for g in range(WIDTH):
        field[g * NODES : (g + 1) * NODES] = rhs_ref[g]
    right = field[...]

    def traces(v_high, v_low):
        both = dot(sel_ref[...], jnp.concatenate([v_high, v_low], axis=1))
        rows = [both[f * ROWS : (f + 1) * ROWS] for f in range(6)]
        return jnp.concatenate(
            [
                jnp.concatenate([row[:, :count] for row in rows], axis=1),
                jnp.concatenate([row[:, count:] for row in rows], axis=1),
            ],
            axis=0,
        ).astype(BF16)

    near_info = []
    xcopies = []

    def turned(values, codes, table):
        high, low = split(values)
        forms = dot(table[...], jnp.concatenate([high, low], axis=0))
        result = forms[:ROWS]
        for code in range(1, 8):
            result = jnp.where(codes == code, forms[code * ROWS : (code + 1) * ROWS], result)
        return result

    def operator(v, turn_number):
        v_high, v_low = split(v)
        picked = dot(traces(v_high, v_low), gather[...])
        picked = picked[:ROWS] + picked[ROWS:]
        own_side = picked[:, cols:]
        if not near_info:
            for k in range(4):
                guarded(k, pcopies[k].wait_recv)
            info = jnp.concatenate([pbuf[k] for k in range(4)], axis=1)
            near_info.append(info[0:1].astype(jnp.int32))
            near_info.append(info[1:2].astype(jnp.int32))
            power = jnp.concatenate([pbuf[k][2:3] for k in range(4)], axis=1)
            diag[:, :cols] = face_mass * power
            diag[:, cols:] = face_mass * strength
        kinds, codes = near_info
        oriented = turned(picked[:, :cols], codes, turn_ref)
        high, low = split(oriented)
        forms = dot(map_high, high) + dot(map_high, low) + dot(map_low, high)
        near_side = jnp.where(kinds == 1, oriented, 0.0)
        for s in range(4):
            near_side = jnp.where(kinds == s + 2, forms[s * ROWS : (s + 1) * ROWS], near_side)
        for k in range(4):
            main, tail = pack(
                near_side[:, k * pad : (k + 1) * pad], own_side[:, (k ^ 1) * pad : ((k ^ 1) + 1) * pad], ghost, pad
            )
            xsrc[turn_number, k, :ROWS] = main
            xsrc[turn_number, k, ROWS:] = tail
        copies = []
        for k in range(4):
            copies.append(pltpu.make_async_remote_copy(
                src_ref=xsrc.at[turn_number, k], dst_ref=xbuf.at[turn_number, k ^ 1],
                send_sem=xsend.at[turn_number, k], recv_sem=xrecv.at[turn_number, k ^ 1],
                device_id=near_device(k), device_id_type=MESH,
            ))
        for k in (2, 3, 0, 1):
            guarded(k, copies[k].start)
        xcopies.append(copies)
        image = dot(vol_ref[:, : 2 * CUBE], jnp.concatenate([v_high, v_low], axis=0))
        image = (image + dot(vol_ref[:, 2 * CUBE :], v_high)) * scale + mass_scale * v
        for k in range(4):
            guarded(k ^ 1, copies[k].wait_recv)
        got = [unpack(xbuf[turn_number, k, :ROWS], xbuf[turn_number, k, ROWS:], ghost, pad) for k in range(4)]
        near_got = jnp.concatenate([got[k][1] for k in range(4)], axis=1)
        own_got = jnp.concatenate([got[k ^ 1][0] for k in range(4)], axis=1)
        near_flux = diag[:, :cols] * (near_side - near_got)
        own_flux = diag[:, cols:] * (own_side - own_got)
        stacked = jnp.concatenate([jnp.where(kinds == s + 2, near_flux, 0.0) for s in range(4)], axis=0)
        high, low = split(stacked)
        near_flux = jnp.where(kinds == 1, near_flux, 0.0)
        near_flux = near_flux + dot(back_twice, jnp.concatenate([high, low], axis=0)) + dot(back_low, high)
        near_flux = turned(near_flux, codes, back_ref)
        flux = jnp.concatenate([near_flux, own_flux], axis=1)
        faces = dot_nt(jnp.concatenate(split(flux), axis=0), gather[...])
        faces = faces[:ROWS] + faces[ROWS:]
        faces = jnp.concatenate([faces[:, f * count : (f + 1) * count] for f in range(6)], axis=0)
        return image + dot(lift_ref[...], jnp.concatenate(split(faces), axis=0))

    def level_copy(turn_number, level, step):
        return pltpu.make_async_remote_copy(
            src_ref=asrc.at[turn_number, level], dst_ref=slots_refs[level].at[turn_number, step - 1],
            send_sem=asend.at[turn_number, level], recv_sem=arecv.at[turn_number, level],
            device_id=peer(level, step), device_id_type=MESH,
        )

    def level_start(turn_number, level):
        def start(step, carry):
            level_copy(turn_number, level, step).start()
            return carry
        lax.fori_loop(1, levels[level][1], start, 0)

    def sums_start(turn_number, pairs):
        lane = lax.broadcasted_iota(jnp.int32, (1, 128), 1)
        row = jnp.zeros((1, 128), F32)
        for i, (a, b) in enumerate(pairs):
            part = jnp.sum(jnp.sum(a * b, axis=0, keepdims=True), axis=1, keepdims=True)
            row = jnp.where(lane == i, part, row)
        asrc[turn_number, 0] = row
        level_start(turn_number, 0)

    def sums_wait(turn_number, number):
        for level in range(len(levels)):
            landed = slots_refs[level].at[turn_number]
            pltpu.make_async_copy(landed, landed, arecv.at[turn_number, level]).wait()
            value = asrc[turn_number, level] + jnp.sum(landed[...], axis=0)
            if level + 1 < len(levels):
                asrc[turn_number, level + 1] = value
                level_start(turn_number, level + 1)
        return [value[:, i : i + 1] for i in range(number)]

    asrc[...] = jnp.zeros_like(asrc)
    r = right
    w = operator(r, 0)
    x = p = s = z = None
    norm_last = None
    for it in range(ITERS):
        pairs = [(r, r), (r, w)]
        if it:
            pairs += [(r, s), (p, w), (p, s)]
        sums_start(it, pairs)
        q = operator(w, it + 1) if it + 1 < ITERS else None
        sums = sums_wait(it, len(pairs))
        norm = sums[0]
        if it == 0:
            alpha = norm / sums[1]
            p, s, z = r, w, q
            x = alpha * p
        else:
            beta = norm / norm_last
            alpha = norm / (sums[1] + beta * (sums[2] + sums[3]) + beta * beta * sums[4])
            p = r + beta * p
            s = w + beta * s
            x = x + alpha * p
            if q is not None:
                z = q + beta * z
        r = r - alpha * s
        if q is not None:
            w = w - alpha * z
        norm_last = norm

    field[...] = x
    for g in range(WIDTH):
        x_out[g] = field[g * NODES : (g + 1) * NODES]
    mapz[...] = r
    for g in range(WIDTH):
        r_out[g] = mapz[g * NODES : (g + 1) * NODES]

    for k in range(4):
        guarded(k ^ 1, pcopies[k].wait_send)
        for copies in xcopies:
            guarded(k, copies[k].wait_send)
    for it in range(ITERS):
        for level in range(len(levels)):
            landed = slots_refs[level].at[it]
            pltpu.make_async_copy(landed, landed, asend.at[it, level]).wait()


def body(n_sfc, n_grp, right_side, cell_level, own_slot, near_slot, face_kind, orientation, penalty, send_slots, maps):
    count = right_side.shape[-1]
    ghost = send_slots.shape[0] // 4
    pad = -(-ghost // 128) * 128
    levels = ring_levels(n_sfc * n_grp)
    vmem = pl.BlockSpec(memory_space=pltpu.VMEM)
    dma = pltpu.SemaphoreType.DMA
    shape = jax.ShapeDtypeStruct((WIDTH, NODES, count), F32)
    x, r = pl.pallas_call(
        functools.partial(kernel, (n_sfc, n_grp, count, ghost, pad)),
        out_shape=(shape, shape),
        in_specs=[vmem] * 15,
        out_specs=(vmem, vmem),
        scratch_shapes=[
            pltpu.VMEM((CUBE, count), F32),
            pltpu.VMEM((6 * count, 8 * pad), BF16),
            pltpu.VMEM((4 * ROWS, 128), F32),
            pltpu.VMEM((ROWS, 8 * pad), F32),
            pltpu.VMEM((4, 8, pad), F32),
            pltpu.VMEM((4, 8, pad), F32),
            pltpu.VMEM((ITERS, 4, ROWS + tail_rows(ghost, pad), pad), F32),
            pltpu.VMEM((ITERS, 4, ROWS + tail_rows(ghost, pad), pad), F32),
            pltpu.VMEM((ITERS, len(levels), 1, 128), F32),
        ]
        + [pltpu.VMEM((ITERS, size - 1, 1, 128), F32) for _, size in levels]
        + [
            dma((4,)),
            dma((4,)),
            dma((ITERS, 4)),
            dma((ITERS, 4)),
            dma((ITERS, len(levels))),
            dma((ITERS, len(levels))),
        ],
        compiler_params=pltpu.CompilerParams(collective_id=0, has_side_effects=True),
    )(
        right_side.reshape(WIDTH, NODES, count),
        cell_level, own_slot, near_slot, face_kind, orientation, penalty, send_slots,
        jnp.swapaxes(maps, 0, 1), *constants(),
    )
    return x.reshape(right_side.shape), r.reshape(right_side.shape)


def solution(mesh):
    split_spec = P(("sfc", "grp"))
    field_spec = P(None, None, None, ("sfc", "grp"))
    return jax.shard_map(
        functools.partial(body, mesh.shape["sfc"], mesh.shape["grp"]),
        mesh=mesh,
        in_specs=(field_spec,) + (split_spec,) * 7 + (P(),),
        out_specs=(field_spec, field_spec),
        check_vma=False,
    )
```
